16 devices in a mesh: rep: 4 (over y, z, core), pp: 4 (over x).
Axes of the slice: x: 4, y: 2, z: 1, core: 2. Of those that a mesh axis runs over, the one named last changes fastest.
The devices are a block of a 4x4x8 slice.
Arguments:
- x: bfloat16 [32, 512, 512], P('rep'), parts along dimension 0
- dy: bfloat16 [32, 512, 512], P('rep'), parts along dimension 0
- w_gate: bfloat16 [4, 512, 1536], P('pp')
- w_up: bfloat16 [4, 512, 1536], P('pp')
- w_down: bfloat16 [4, 1536, 512], P('pp')
Outputs:
- output 1: bfloat16 [16, 512, 1536], P(('rep', 'pp')), parts along dimension 0
- output 2: bfloat16 [16, 512, 1536], P(('rep', 'pp')), parts along dimension 0
- output 3: bfloat16 [16, 1536, 512], P(('rep', 'pp')), parts along dimension 0
There are 4 independent parts. The reference program is written for one: setup_inputs(seed, part) draws one part's arguments, and reference() takes and returns one part's arrays. A program takes and returns all parts, laid end to end along the dimension named above; an argument that names none is the same for every part.
All inputs are finite; a program needn't handle non-finite values.
Results may differ from the reference program's by a relative error of at most 0.0181.
Values are sent between devices in bfloat16 or wider.
A program may use at most 768 MiB of HBM per device.

```python
import jax
import jax.numpy as jnp
from jax import lax

MICRO = 8
TOKENS = 512
D = 512
FF = 1536
LAYERS = 4
NAMES = ("w_gate", "w_up", "w_down")
SHAPES = {"w_gate": (LAYERS, D, FF), "w_up": (LAYERS, D, FF), "w_down": (LAYERS, FF, D)}


def bump(key, n, height):
    away = (jnp.arange(n, dtype=jnp.int32) - jax.random.randint(key, (), 0, n, jnp.int32)) % n
    return jnp.where(away < n // 8, height, 1.0)


def together(key, own, strength):
    shared = jax.random.normal(key, own.shape[1:], jnp.float32)
    return (own + strength * shared) * lax.rsqrt(1 + strength * strength)


def setup_inputs(seed: int = 0, part: int = 0) -> dict:
    kx, kdy, ka, kb, kz, kf, kh, kl, *kw = jax.random.split(jax.random.key(seed), 8 + len(NAMES))
    kx, kdy, ka, kb = (jax.random.fold_in(k, part) for k in (kx, kdy, ka, kb))
    shape = (MICRO, TOKENS, D)
    much_x, much_dy = jax.random.uniform(kz, (2,), jnp.float32, 0.0, 1.0)
    layers = 2.0 ** jax.random.uniform(kl, (LAYERS, 1, 1), jnp.float32, -1.0, 1.0)
    x = together(ka, jax.random.normal(kx, shape, jnp.float32), much_x) * bump(kf, D, 4.0)
    dy = together(kb, jax.random.normal(kdy, shape, jnp.float32), much_dy)
    drawn = {"x": x.astype(jnp.bfloat16), "dy": (dy * (MICRO * TOKENS) ** -0.5).astype(jnp.bfloat16)}
    for key, name in zip(kw, NAMES, strict=True):
        w = jax.random.normal(key, SHAPES[name], jnp.float32) * SHAPES[name][1] ** -0.5
        drawn[name] = (w * {"w_gate": 1.0, "w_up": bump(kh, FF, 4.0), "w_down": layers}[name]).astype(jnp.bfloat16)
    return drawn


def matmul(a, w):
    return jnp.dot(a, w, preferred_element_type=jnp.float32).astype(jnp.bfloat16)


def normed(h):
    wide = h.astype(jnp.float32)
    scale = lax.rsqrt(jnp.mean(wide**2, -1, keepdims=True) + 1e-6)
    return (wide * scale).astype(jnp.bfloat16)


def layer(h, w):
    a = normed(h)
    gate = jnp.dot(a, w["w_gate"], preferred_element_type=jnp.float32)
    up = jnp.dot(a, w["w_up"], preferred_element_type=jnp.float32)
    return h + matmul((jax.nn.silu(gate) * up).astype(jnp.bfloat16), w["w_down"])


def stack(weights, h):
    return lax.scan(lambda h, w: (layer(h, w), None), h, weights)[0]


def reference(x, dy, w_gate, w_up, w_down):
    weights = dict(zip(NAMES, (w_gate, w_up, w_down), strict=True))

    def take(so_far, one):
        h, by_y = one
        _, back = jax.vjp(lambda w: stack(w, h), weights)
        return jax.tree.map(lambda total, term: total + term.astype(jnp.float32), so_far, back(by_y)[0]), None

    none_yet = {name: jnp.zeros(w.shape, jnp.float32) for name, w in weights.items()}
    by_weights, _ = lax.scan(take, none_yet, (x, dy))
    return tuple(by_weights[name].astype(jnp.bfloat16) for name in NAMES)
```

```python
import functools

import jax
import jax.numpy as jnp
from jax import lax
from jax.experimental import pallas as pl
from jax.experimental.pallas import tpu as pltpu
from jax.sharding import PartitionSpec as P

F32, BF16 = jnp.float32, jnp.bfloat16
ROWS = 128
LAG = 4
SLOTS = 14
RING = 6
LANES = 128


def dot(a, b):
    return jnp.dot(a, b, preferred_element_type=F32)


def dot_tokens(a, b):
    return lax.dot_general(a, b, (((0,), (0,)), ((), ())), preferred_element_type=F32)


def scale_of(wide):
    return lax.rsqrt(jnp.mean(wide * wide, -1, keepdims=True) + 1e-6)


def sigmoid(v):
    return 0.5 * jnp.tanh(0.5 * v) + 0.5


def transpose_down(wd, wdt):
    @pl.loop(0, wd.shape[0] // LANES)
    def _(i):
        part = pl.ds(pl.multiple_of(i * LANES, LANES), LANES)
        wdt[:, part] = wd[part, :].T


def transpose_gate_up(wgu, wgut):
    @pl.loop(0, wgu.shape[1] // LANES)
    def _(i):
        part = pl.ds(pl.multiple_of(i * LANES, LANES), LANES)
        wgut[part, :] = wgu[:, part].T


def forward_chunk(hc, wgu, wd, keep, onward, out):
    ff = wd.shape[0]
    wide = hc.astype(F32)
    a = (wide * scale_of(wide)).astype(BF16)
    if not onward:
        keep[...] = dot(a, wgu[...])
        return
    acts = []
    width = ff // 3
    for i in range(3):
        lo, hi = i * width, (i + 1) * width
        gate = dot(a, wgu[:, lo:hi])
        up = dot(a, wgu[:, ff + lo : ff + hi])
        keep[:, lo:hi] = gate
        keep[:, ff + lo : ff + hi] = up
        acts.append((gate * sigmoid(gate) * up).astype(BF16))
    act = jnp.concatenate(acts, axis=1)
    out[...] = hc + dot(act, wd[...]).astype(BF16)


def backward_chunk(hc, gc, wdt, wgut, keep, a_out, act_out, dgu_out, onward, out):
    ff = wdt.shape[1]
    wide = hc.astype(F32)
    scale = scale_of(wide)
    a_out[...] = (wide * scale).astype(BF16)
    gates, ups = [], []
    width = ff // 3
    for i in range(3):
        lo, hi = i * width, (i + 1) * width
        d = dot(gc, wdt[:, lo:hi]).astype(BF16).astype(F32)
        gate, up = keep[:, lo:hi], keep[:, ff + lo : ff + hi]
        sig = sigmoid(gate)
        silu = gate * sig
        act_out[:, lo:hi] = (silu * up).astype(BF16)
        by_up = (d * silu).astype(BF16)
        by_gate = (d * up * (sig + silu * (1.0 - sig))).astype(BF16)
        dgu_out[:, lo:hi] = by_gate
        dgu_out[:, ff + lo : ff + hi] = by_up
        gates.append(by_gate)
        ups.append(by_up)
    if not onward:
        return
    by_a = dot(jnp.concatenate(gates, axis=1), wgut[:ff, :]).astype(BF16) + dot(jnp.concatenate(ups, axis=1), wgut[ff:, :]).astype(BF16)
    by_a = by_a.astype(F32)
    inner = jnp.sum(by_a * wide, -1, keepdims=True) * (scale * scale * scale * (1.0 / wide.shape[-1]))
    out[...] = gc + (by_a * scale - wide * inner).astype(BF16)


def weight_terms(a, g, dgu, act):
    return dot_tokens(a, dgu).astype(BF16).astype(F32), dot_tokens(g, act).astype(BF16).astype(F32)


def kernel(
    stages,
    micro,
    tokens,
    x,
    dy,
    w_gate,
    w_up,
    w_down,
    o_gate,
    o_up,
    o_down,
    wgu,
    wd,
    wgut,
    wdt,
    h,
    g,
    hs,
    gs,
    keep,
    a_keep,
    act_keep,
    dgu_keep,
    acc_gu,
    acc_d,
    w_sem,
    o_sem,
    h_recv,
    g_recv,
    h_send,
    g_send,
):
    me = lax.axis_index("pp")
    first, last = me == 0, me == stages - 1
    ff = wd.shape[0]
    per = tokens // ROWS
    chunks = micro * per
    band = wgu.shape[0] // per
    lag = LAG * (stages - 1 - me)

    def rows_of(c):
        return pl.ds(pl.multiple_of(c * ROWS, ROWS), ROWS)

    def from_x(c):
        return pltpu.make_async_copy(x.at[rows_of(c)], h.at[rows_of(c)], h_recv.at[c])

    def from_dy(c):
        return pltpu.make_async_copy(dy.at[rows_of(c)], g.at[rows_of(c)], g_recv.at[c])

    def send_h(c):
        slot = lax.rem(c, RING)
        return pltpu.make_async_remote_copy(
            src_ref=hs.at[slot],
            dst_ref=h.at[rows_of(c)],
            send_sem=h_send.at[slot],
            recv_sem=h_recv.at[c],
            device_id={"pp": lax.rem(me + 1, stages)},
            device_id_type=pl.DeviceIdType.MESH,
        )

    def send_g(c):
        slot = lax.rem(c, RING)
        return pltpu.make_async_remote_copy(
            src_ref=gs.at[slot],
            dst_ref=g.at[rows_of(c)],
            send_sem=g_send.at[slot],
            recv_sem=g_recv.at[c],
            device_id={"pp": lax.rem(me + stages - 1, stages)},
            device_id_type=pl.DeviceIdType.MESH,
        )

    @pl.when(first)
    def _():
        from_x(0).start()

    loads = (
        pltpu.make_async_copy(w_gate, wgu.at[:, pl.ds(0, ff)], w_sem.at[0]),
        pltpu.make_async_copy(w_up, wgu.at[:, pl.ds(ff, ff)], w_sem.at[1]),
        pltpu.make_async_copy(w_down, wd, w_sem.at[2]),
    )
    for load in loads:
        load.start()

    barrier = pltpu.get_barrier_semaphore()
    for other in (lax.rem(me + 1, stages), lax.rem(me + stages - 1, stages)):
        pl.semaphore_signal(barrier, inc=1, device_id={"pp": other}, device_id_type=pl.DeviceIdType.MESH)

    @pl.when(first)
    def _():
        @pl.loop(1, chunks)
        def _(c):
            from_x(c).start()

    @pl.when(last)
    def _():
        @pl.loop(0, chunks)
        def _(c):
            from_dy(c).start()

    acc_gu[...] = jnp.zeros_like(acc_gu)
    acc_d[...] = jnp.zeros_like(acc_d)
    for load in loads:
        load.wait()

    @pl.when(jnp.logical_not(first))
    def _():
        transpose_gate_up(wgu, wgut)
        transpose_down(wd, wdt)

    pl.semaphore_wait(barrier, 2)

    def out_copies(j):
        slot = (micro - 2) % 2
        rows = pl.ds(pl.multiple_of(j * band, band), band)
        return (
            pltpu.make_async_copy(dgu_keep.at[slot, rows, pl.ds(0, ff)], o_gate.at[rows], o_sem.at[0, j]),
            pltpu.make_async_copy(dgu_keep.at[slot, rows, pl.ds(ff, ff)], o_up.at[rows], o_sem.at[1, j]),
            pltpu.make_async_copy(act_keep.at[slot, rows], o_down.at[rows], o_sem.at[2, j]),
        )

    @pl.loop(0, chunks + LAG * (stages - 1) + per - 1)
    def _(t):
        @pl.when(t < chunks)
        def _():
            c = t
            slot = lax.rem(c, SLOTS)

            @pl.when(first)
            def _():
                from_x(c).wait()

            @pl.when(jnp.logical_not(first))
            def _():
                send_h(c).wait_recv()

            @pl.when(last)
            def _():
                forward_chunk(h[rows_of(c), :], wgu, wd, keep.at[slot], False, None)

            @pl.when(jnp.logical_not(last))
            def _():
                @pl.when(c >= RING)
                def _():
                    send_h(c).wait_send()

                forward_chunk(h[rows_of(c), :], wgu, wd, keep.at[slot], True, hs.at[lax.rem(c, RING)])
                send_h(c).start()

        @pl.when(jnp.logical_and(first, t == 2))
        def _():
            transpose_down(wd, wdt)

        @pl.when(jnp.logical_and(t >= lag, t < chunks + lag))
        def _():
            c = t - lag
            slot, half = lax.rem(c, SLOTS), lax.rem(lax.div(c, per), 2)
            inside = rows_of(lax.rem(c, per))

            @pl.when(last)
            def _():
                from_dy(c).wait()

            @pl.when(jnp.logical_not(last))
            def _():
                send_g(c).wait_recv()

            parts = (
                h[rows_of(c), :],
                g[rows_of(c), :],
                wdt,
                wgut,
                keep.at[slot],
                a_keep.at[half, inside],
                act_keep.at[half, inside],
                dgu_keep.at[half, inside],
            )

            @pl.when(first)
            def _():
                backward_chunk(*parts, False, None)

            @pl.when(jnp.logical_not(first))
            def _():
                @pl.when(c >= RING)
                def _():
                    send_g(c).wait_send()

                backward_chunk(*parts, True, gs.at[lax.rem(c, RING)])
                send_g(c).start()

        u = t - lag - (per - 1)

        @pl.when(jnp.logical_and(u >= 0, u < chunks))
        def _():
            m, j = lax.div(u, per), lax.rem(u, per)
            half = lax.rem(m, 2)
            rows = pl.ds(pl.multiple_of(j * band, band), band)
            by_gu, by_d = weight_terms(
                a_keep[half, :, rows],
                g[pl.ds(pl.multiple_of(m * tokens, tokens), tokens), rows],
                dgu_keep[half],
                act_keep[half],
            )

            @pl.when(m < micro - 1)
            def _():
                acc_gu[rows, :] += by_gu
                acc_d[rows, :] += by_d

            @pl.when(m == micro - 1)
            def _():
                other = (micro - 2) % 2
                dgu_keep[other, rows, :] = (acc_gu[rows, :] + by_gu).astype(BF16)
                act_keep[other, rows, :] = (acc_d[rows, :] + by_d).astype(BF16)
                for copy in out_copies(j):
                    copy.start()

    @pl.loop(0, min(RING, chunks))
    def _(c):
        @pl.when(jnp.logical_not(last))
        def _():
            send_h(c).wait_send()

        @pl.when(jnp.logical_not(first))
        def _():
            send_g(c).wait_send()

    @pl.loop(0, per)
    def _(j):
        for copy in out_copies(j):
            copy.wait()


def solution(mesh):
    stages = mesh.shape["pp"]

    def step(x, dy, w_gate, w_up, w_down):
        micro, tokens, d = x.shape
        ff = w_gate.shape[-1]
        assert w_gate.shape[0] == 1
        per = tokens // ROWS
        chunks = micro * per
        anywhere = pl.BlockSpec(memory_space=pl.ANY)
        tall = jax.ShapeDtypeStruct((d, ff), BF16)
        by_gate, by_up, by_down = pl.pallas_call(
            functools.partial(kernel, stages, micro, tokens),
            out_shape=(tall, tall, tall),
            in_specs=[anywhere] * 5,
            out_specs=(anywhere,) * 3,
            scratch_shapes=[
                pltpu.VMEM((d, 2 * ff), BF16),
                pltpu.VMEM((ff, d), BF16),
                pltpu.VMEM((2 * ff, d), BF16),
                pltpu.VMEM((d, ff), BF16),
                pltpu.VMEM((micro * tokens, d), BF16),
                pltpu.VMEM((micro * tokens, d), BF16),
                pltpu.VMEM((RING, ROWS, d), BF16),
                pltpu.VMEM((RING, ROWS, d), BF16),
                pltpu.VMEM((SLOTS, ROWS, 2 * ff), F32),
                pltpu.VMEM((2, tokens, d), BF16),
                pltpu.VMEM((2, tokens, ff), BF16),
                pltpu.VMEM((2, tokens, 2 * ff), BF16),
                pltpu.VMEM((d, 2 * ff), F32),
                pltpu.VMEM((d, ff), F32),
                pltpu.SemaphoreType.DMA((3,)),
                pltpu.SemaphoreType.DMA((3, per)),
                pltpu.SemaphoreType.DMA((chunks,)),
                pltpu.SemaphoreType.DMA((chunks,)),
                pltpu.SemaphoreType.DMA((RING,)),
                pltpu.SemaphoreType.DMA((RING,)),
            ],
            compiler_params=pltpu.CompilerParams(collective_id=0, has_side_effects=True, vmem_limit_bytes=67043328),
        )(x.reshape(micro * tokens, d), dy.reshape(micro * tokens, d), w_gate[0], w_up[0], w_down[0])
        return by_gate[None], by_up[None], by_down.T[None]

    return jax.shard_map(
        step,
        mesh=mesh,
        in_specs=(P("rep", None, None),) * 2 + (P("pp", None, None),) * 3,
        out_specs=(P(("rep", "pp"), None, None),) * 3,
        check_vma=False,
    )
```

```python
import functools

import jax
import jax.numpy as jnp
from jax import lax
from jax.experimental import pallas as pl
from jax.experimental.pallas import tpu as pltpu
from jax.sharding import PartitionSpec as P

F32, BF16 = jnp.float32, jnp.bfloat16
ROWS = 128
LAGS = (0, 4, 8, 12)
SLOTS = max(LAGS) + 1
RING = 5
LANES = 128


def dot(a, b):
    return jnp.dot(a, b, preferred_element_type=F32)


def dot_tokens(a, b):
    return lax.dot_general(a, b, (((0,), (0,)), ((), ())), preferred_element_type=F32)


def scale_of(wide):
    return lax.rsqrt(jnp.mean(wide * wide, -1, keepdims=True) + 1e-6)


def sigmoid(v):
    return 0.5 * jnp.tanh(0.5 * v) + 0.5


def transpose_down(wd, wdt):
    @pl.loop(0, wd.shape[0] // LANES)
    def _(i):
        part = pl.ds(pl.multiple_of(i * LANES, LANES), LANES)
        wdt[:, part] = wd[part, :].T


def transpose_gate_up(wgu, wgut):
    @pl.loop(0, wgu.shape[1] // LANES)
    def _(i):
        part = pl.ds(pl.multiple_of(i * LANES, LANES), LANES)
        wgut[part, :] = wgu[:, part].T


def forward_chunk(hc, wgu, wd, keep, act_out, out):
    ff = wd.shape[0]
    wide = hc.astype(F32)
    a = (wide * scale_of(wide)).astype(BF16)
    acts = []
    width = ff // 6
    for i in range(6):
        lo, hi = i * width, (i + 1) * width
        gate = dot(a, wgu[:, lo:hi])
        up = dot(a, wgu[:, ff + lo : ff + hi])
        sig = sigmoid(gate)
        silu = gate * sig
        act = (silu * up).astype(BF16)
        act_out[:, lo:hi] = act
        keep[:, lo:hi] = up * (sig + silu * (1.0 - sig))
        keep[:, ff + lo : ff + hi] = silu
        acts.append(act)
    if out is not None:
        out[...] = hc + dot(jnp.concatenate(acts, axis=1), wd[...]).astype(BF16)


def backward_chunk(hc, gc, wdt, wgut, keep, a_out, dgu_out, out):
    ff = wdt.shape[1]
    wide = hc.astype(F32)
    scale = scale_of(wide)
    a_out[...] = (wide * scale).astype(BF16)
    gates, ups = [], []
    width = ff // 3
    for i in range(3):
        lo, hi = i * width, (i + 1) * width
        d = dot(gc, wdt[:, lo:hi]).astype(BF16).astype(F32)
        by_gate = (d * keep[:, lo:hi]).astype(BF16)
        by_up = (d * keep[:, ff + lo : ff + hi]).astype(BF16)
        dgu_out[:, lo:hi] = by_gate
        dgu_out[:, ff + lo : ff + hi] = by_up
        gates.append(by_gate)
        ups.append(by_up)
    if out is None:
        return
    by_a = dot(jnp.concatenate(gates, axis=1), wgut[:ff, :]).astype(BF16) + dot(jnp.concatenate(ups, axis=1), wgut[ff:, :]).astype(BF16)
    by_a = by_a.astype(F32)
    inner = jnp.sum(by_a * wide, -1, keepdims=True) * (scale * scale * scale * (1.0 / wide.shape[-1]))
    out[...] = gc + (by_a * scale - wide * inner).astype(BF16)


def weight_terms(a, g, dgu, act):
    return dot_tokens(a, dgu).astype(BF16).astype(F32), dot_tokens(act, g).astype(BF16).astype(F32)


def kernel(
    stages,
    micro,
    tokens,
    x,
    dy,
    w_gate,
    w_up,
    w_down,
    o_gate,
    o_up,
    o_down,
    wgu,
    wd,
    wgut,
    wdt,
    h,
    g,
    hs,
    gs,
    keep,
    a_keep,
    act_keep,
    dgu_keep,
    acc_gu,
    acc_d,
    w_sem,
    o_sem,
    h_recv,
    g_recv,
    h_send,
    g_send,
):
    me = lax.axis_index("pp")
    first, last = me == 0, me == stages - 1
    ff = wd.shape[0]
    per = tokens // ROWS
    chunks = micro * per
    d = wgu.shape[0]
    band, tall = d // per, ff // per
    pieces = ff // d
    behind = stages - 1 - me
    lag = sum(jnp.where(behind == i, LAGS[i], 0) for i in range(stages))
    blocks = act_keep.shape[0]

    def rows_of(c):
        return pl.ds(pl.multiple_of(c * ROWS, ROWS), ROWS)

    def from_x(c):
        return pltpu.make_async_copy(x.at[rows_of(c)], h.at[rows_of(c)], h_recv.at[c])

    def from_dy(c):
        return pltpu.make_async_copy(dy.at[rows_of(c)], g.at[rows_of(c)], g_recv.at[c])

    def send_h(c):
        slot = lax.rem(c, RING)
        return pltpu.make_async_remote_copy(
            src_ref=hs.at[slot],
            dst_ref=h.at[rows_of(c)],
            send_sem=h_send.at[slot],
            recv_sem=h_recv.at[c],
            device_id={"pp": lax.rem(me + 1, stages)},
            device_id_type=pl.DeviceIdType.MESH,
        )

    def send_g(c):
        slot = lax.rem(c, RING)
        return pltpu.make_async_remote_copy(
            src_ref=gs.at[slot],
            dst_ref=g.at[rows_of(c)],
            send_sem=g_send.at[slot],
            recv_sem=g_recv.at[c],
            device_id={"pp": lax.rem(me + stages - 1, stages)},
            device_id_type=pl.DeviceIdType.MESH,
        )

    @pl.when(first)
    def _():
        from_x(0).start()

    loads = (
        pltpu.make_async_copy(w_gate, wgu.at[:, pl.ds(0, ff)], w_sem.at[0]),
        pltpu.make_async_copy(w_up, wgu.at[:, pl.ds(ff, ff)], w_sem.at[1]),
        pltpu.make_async_copy(w_down, wd, w_sem.at[2]),
    )
    for load in loads:
        load.start()

    barrier = pltpu.get_barrier_semaphore()
    for other in (lax.rem(me + 1, stages), lax.rem(me + stages - 1, stages)):
        pl.semaphore_signal(barrier, inc=1, device_id={"pp": other}, device_id_type=pl.DeviceIdType.MESH)

    @pl.when(first)
    def _():
        @pl.loop(1, chunks)
        def _(c):
            from_x(c).start()

    @pl.when(last)
    def _():
        @pl.loop(0, chunks)
        def _(c):
            from_dy(c).start()

    def clear():
        acc_gu[...] = jnp.zeros_like(acc_gu)
        acc_d[...] = jnp.zeros_like(acc_d)

    for load in loads:
        load.wait()

    @pl.when(jnp.logical_not(first))
    def _():
        clear()
        transpose_gate_up(wgu, wgut)
        transpose_down(wd, wdt)

    pl.semaphore_wait(barrier, 2)

    def out_copies(j):
        slot = (micro - 2) % 2
        rows = pl.ds(pl.multiple_of(j * band, band), band)
        return (
            pltpu.make_async_copy(dgu_keep.at[slot, rows, pl.ds(0, ff)], o_gate.at[rows], o_sem.at[0, j]),
            pltpu.make_async_copy(dgu_keep.at[slot, rows, pl.ds(ff, ff)], o_up.at[rows], o_sem.at[1, j]),
        ) + tuple(
            pltpu.make_async_copy(
                act_keep.at[(micro - 2) % blocks, rows, pl.ds(i * d, d)],
                o_down.at[pl.ds(pl.multiple_of(j * tall + i * band, band), band)],
                o_sem.at[2 + i, j],
            )
            for i in range(pieces)
        )

    @pl.loop(0, chunks + LAGS[stages - 1] + per - 1)
    def _(t):
        @pl.when(t < chunks)
        def _():
            c = t
            slot = lax.rem(c, SLOTS)
            act_out = act_keep.at[lax.rem(lax.div(c, per), blocks), rows_of(lax.rem(c, per))]

            @pl.when(first)
            def _():
                from_x(c).wait()

            @pl.when(jnp.logical_not(first))
            def _():
                send_h(c).wait_recv()

            @pl.when(last)
            def _():
                forward_chunk(h[rows_of(c), :], wgu, wd, keep.at[slot], act_out, None)

            @pl.when(jnp.logical_not(last))
            def _():
                @pl.when(c >= RING)
                def _():
                    send_h(c).wait_send()

                forward_chunk(h[rows_of(c), :], wgu, wd, keep.at[slot], act_out, hs.at[lax.rem(c, RING)])
                send_h(c).start()

        @pl.when(jnp.logical_and(first, t == 2))
        def _():
            transpose_down(wd, wdt)

        @pl.when(jnp.logical_and(first, t == 3))
        def _():
            clear()

        @pl.when(jnp.logical_and(t >= lag, t < chunks + lag))
        def _():
            c = t - lag
            slot, half = lax.rem(c, SLOTS), lax.rem(lax.div(c, per), 2)
            inside = rows_of(lax.rem(c, per))

            @pl.when(last)
            def _():
                from_dy(c).wait()

            @pl.when(jnp.logical_not(last))
            def _():
                send_g(c).wait_recv()

            parts = (
                h[rows_of(c), :],
                g[rows_of(c), :],
                wdt,
                wgut,
                keep.at[slot],
                a_keep.at[half, inside],
                dgu_keep.at[half, inside],
            )

            @pl.when(first)
            def _():
                backward_chunk(*parts, None)

            @pl.when(jnp.logical_not(first))
            def _():
                @pl.when(c >= RING)
                def _():
                    send_g(c).wait_send()

                backward_chunk(*parts, gs.at[lax.rem(c, RING)])
                send_g(c).start()

        u = t - lag - (per - 1)

        @pl.when(jnp.logical_and(u >= 0, u < chunks))
        def _():
            m, j = lax.div(u, per), lax.rem(u, per)
            half = lax.rem(m, 2)
            rows = pl.ds(pl.multiple_of(j * band, band), band)
            tall_rows = pl.ds(pl.multiple_of(j * tall, tall), tall)
            by_gu, by_d = weight_terms(
                a_keep[half, :, rows],
                g[pl.ds(pl.multiple_of(m * tokens, tokens), tokens), :],
                dgu_keep[half],
                act_keep[lax.rem(m, blocks), :, tall_rows],
            )

            @pl.when(m < micro - 1)
            def _():
                acc_gu[rows, :] += by_gu
                acc_d[tall_rows, :] += by_d

            @pl.when(m == micro - 1)
            def _():
                dgu_keep[(micro - 2) % 2, rows, :] = (acc_gu[rows, :] + by_gu).astype(BF16)
                total = (acc_d[tall_rows, :] + by_d).astype(BF16)
                for i in range(pieces):
                    act_keep[(micro - 2) % blocks, rows, i * d : (i + 1) * d] = total[i * band : (i + 1) * band, :]
                for copy in out_copies(j):
                    copy.start()

    @pl.loop(0, min(RING, chunks))
    def _(c):
        @pl.when(jnp.logical_not(last))
        def _():
            send_h(c).wait_send()

        @pl.when(jnp.logical_not(first))
        def _():
            send_g(c).wait_send()

    @pl.loop(0, per)
    def _(j):
        for copy in out_copies(j):
            copy.wait()


def hand_over(per, *refs):
    ins, outs, held, sem = refs[:3], refs[3:6], refs[6:9], refs[9]
    moves = []
    for j in range(per):
        for i in range(3):
            size = ins[i].shape[0] // per
            rows = pl.ds(j * size, size)
            moves.append(
                (
                    pltpu.make_async_copy(ins[i].at[rows], held[i].at[0, rows], sem.at[0, i, j]),
                    pltpu.make_async_copy(held[i].at[0, rows], outs[i].at[0, rows], sem.at[1, i, j]),
                )
            )
    for take, _ in moves:
        take.start()
    for take, put in moves:
        take.wait()
        put.start()
    for _, put in moves:
        put.wait()


def solution(mesh):
    stages = mesh.shape["pp"]

    def step(x, dy, w_gate, w_up, w_down):
        micro, tokens, d = x.shape
        ff = w_gate.shape[-1]
        assert w_gate.shape[0] == 1
        per = tokens // ROWS
        chunks = micro * per
        blocks = pl.cdiv(LAGS[stages - 1] + 2 * per, per)
        anywhere = pl.BlockSpec(memory_space=pl.ANY)
        tall = jax.ShapeDtypeStruct((d, ff), BF16)
        by_gate, by_up, by_down = pl.pallas_call(
            functools.partial(kernel, stages, micro, tokens),
            out_shape=(tall, tall, jax.ShapeDtypeStruct((ff, d), BF16)),
            in_specs=[anywhere] * 5,
            out_specs=(anywhere,) * 3,
            scratch_shapes=[
                pltpu.VMEM((d, 2 * ff), BF16),
                pltpu.VMEM((ff, d), BF16),
                pltpu.VMEM((2 * ff, d), BF16),
                pltpu.VMEM((d, ff), BF16),
                pltpu.VMEM((micro * tokens, d), BF16),
                pltpu.VMEM((micro * tokens, d), BF16),
                pltpu.VMEM((RING, ROWS, d), BF16),
                pltpu.VMEM((RING, ROWS, d), BF16),
                pltpu.VMEM((SLOTS, ROWS, 2 * ff), F32),
                pltpu.VMEM((2, tokens, d), BF16),
                pltpu.VMEM((blocks, tokens, ff), BF16),
                pltpu.VMEM((2, tokens, 2 * ff), BF16),
                pltpu.VMEM((d, 2 * ff), F32),
                pltpu.VMEM((ff, d), F32),
                pltpu.SemaphoreType.DMA((3,)),
                pltpu.SemaphoreType.DMA((2 + ff // d, per)),
                pltpu.SemaphoreType.DMA((chunks,)),
                pltpu.SemaphoreType.DMA((chunks,)),
                pltpu.SemaphoreType.DMA((RING,)),
                pltpu.SemaphoreType.DMA((RING,)),
            ],
            compiler_params=pltpu.CompilerParams(collective_id=0, has_side_effects=True, vmem_limit_bytes=67043328),
        )(x.reshape(micro * tokens, d), dy.reshape(micro * tokens, d), w_gate[0], w_up[0], w_down[0])
        shapes = ((1, d, ff), (1, d, ff), (1, ff, d))
        return pl.pallas_call(
            functools.partial(hand_over, per),
            out_shape=tuple(jax.ShapeDtypeStruct(shape, BF16) for shape in shapes),
            in_specs=[anywhere] * 3,
            out_specs=(anywhere,) * 3,
            scratch_shapes=[pltpu.VMEM(shape, BF16) for shape in shapes] + [pltpu.SemaphoreType.DMA((2, 3, per))],
        )(by_gate, by_up, by_down)

    return jax.shard_map(
        step,
        mesh=mesh,
        in_specs=(P("rep", None, None),) * 2 + (P("pp", None, None),) * 3,
        out_specs=(P(("rep", "pp"), None, None),) * 3,
        check_vma=False,
    )
```

```python
import functools

import jax
import jax.numpy as jnp
from jax import lax
from jax.experimental import pallas as pl
from jax.experimental.pallas import tpu as pltpu
from jax.sharding import PartitionSpec as P

F32, BF16 = jnp.float32, jnp.bfloat16
ROWS = 128
LAGS = (0, 4, 8, 13)
SLOTS = max(LAGS) + 1
RING = 3
LANES = 128


def dot(a, b):
    return jnp.dot(a, b, preferred_element_type=F32)


def dot_tokens(a, b):
    return lax.dot_general(a, b, (((0,), (0,)), ((), ())), preferred_element_type=F32)


def scale_of(wide):
    return lax.rsqrt(jnp.mean(wide * wide, -1, keepdims=True) + 1e-6)


def sigmoid(v):
    return 0.5 * jnp.tanh(0.5 * v) + 0.5


def transpose_down(wd, wdt):
    @pl.loop(0, wd.shape[0] // LANES)
    def _(i):
        part = pl.ds(pl.multiple_of(i * LANES, LANES), LANES)
        wdt[:, part] = wd[part, :].T


def transpose_gate_up(wgu, wgut):
    @pl.loop(0, wgu.shape[1] // LANES)
    def _(i):
        part = pl.ds(pl.multiple_of(i * LANES, LANES), LANES)
        wgut[part, :] = wgu[:, part].T


def forward_chunk(hc, wgu, wd, keep, act_out, out):
    ff = wd.shape[0]
    wide = hc.astype(F32)
    a = (wide * scale_of(wide)).astype(BF16)
    acts = []
    width = ff // 6
    for i in range(6):
        lo, hi = i * width, (i + 1) * width
        gate = dot(a, wgu[:, lo:hi])
        up = dot(a, wgu[:, ff + lo : ff + hi])
        sig = sigmoid(gate)
        silu = gate * sig
        act = (silu * up).astype(BF16)
        act_out[:, lo:hi] = act
        keep[:, lo:hi] = up * (sig + silu * (1.0 - sig))
        keep[:, ff + lo : ff + hi] = silu
        acts.append(act)
    if out is not None:
        out[...] = hc + dot(jnp.concatenate(acts, axis=1), wd[...]).astype(BF16)


def backward_chunk(hc, gc, wdt, wgut, keep, a_out, dgu_out, out):
    ff = wdt.shape[1]
    wide = hc.astype(F32)
    scale = scale_of(wide)
    gates, ups = [], []
    width = ff // 3
    for i in range(3):
        lo, hi = i * width, (i + 1) * width
        d = dot(gc, wdt[:, lo:hi]).astype(BF16).astype(F32)
        by_gate = (d * keep[:, lo:hi]).astype(BF16)
        by_up = (d * keep[:, ff + lo : ff + hi]).astype(BF16)
        dgu_out[:, lo:hi] = by_gate
        dgu_out[:, ff + lo : ff + hi] = by_up
        gates.append(by_gate)
        ups.append(by_up)
    a_out[...] = (wide * scale).astype(BF16)
    if out is not None:
        send_back(gc, wide, scale, gates, ups, wgut, out)


def both_ways_chunk(hc, gc, wgu, wdt, wgut, a_out, act_out, dgu_out, out):
    ff = wdt.shape[1]
    wide = hc.astype(F32)
    scale = scale_of(wide)
    a = (wide * scale).astype(BF16)
    gates, ups = [], []
    width = ff // 6
    for i in range(6):
        lo, hi = i * width, (i + 1) * width
        gate = dot(a, wgu[:, lo:hi])
        up = dot(a, wgu[:, ff + lo : ff + hi])
        d = dot(gc, wdt[:, lo:hi]).astype(BF16).astype(F32)
        sig = sigmoid(gate)
        silu = gate * sig
        act_out[:, lo:hi] = (silu * up).astype(BF16)
        by_gate = (d * (up * (sig + silu * (1.0 - sig)))).astype(BF16)
        by_up = (d * silu).astype(BF16)
        dgu_out[:, lo:hi] = by_gate
        dgu_out[:, ff + lo : ff + hi] = by_up
        gates.append(by_gate)
        ups.append(by_up)
    a_out[...] = a
    send_back(gc, wide, scale, gates, ups, wgut, out)


def send_back(gc, wide, scale, gates, ups, wgut, out):
    half = wgut.shape[0] // 2
    by_a = dot(jnp.concatenate(gates, axis=1), wgut[:half, :]).astype(BF16) + dot(jnp.concatenate(ups, axis=1), wgut[half:, :]).astype(BF16)
    by_a = by_a.astype(F32)
    inner = jnp.sum(by_a * wide, -1, keepdims=True) * (scale * scale * scale * (1.0 / wide.shape[-1]))
    out[...] = gc + (by_a * scale - wide * inner).astype(BF16)


def kernel(
    stages,
    micro,
    tokens,
    x,
    dy,
    w_gate,
    w_up,
    w_down,
    o_gate,
    o_up,
    o_down,
    wgu,
    wd,
    wgut,
    wdt,
    h,
    g,
    hs,
    gs,
    keep,
    act_keep,
    dgu_keep,
    acc_gu,
    acc_d,
    w_sem,
    o_sem,
    h_recv,
    g_recv,
    h_send,
    g_send,
):
    me = lax.axis_index("pp")
    first, last = me == 0, me == stages - 1
    ff = wd.shape[0]
    per = tokens // ROWS
    chunks = micro * per
    d = wgu.shape[0]
    band, tall = d // per, ff // per
    pieces = ff // d
    behind = stages - 1 - me
    lag = sum(jnp.where(behind == i, LAGS[i], 0) for i in range(stages))
    blocks = act_keep.shape[0]

    def rows_of(c):
        return pl.ds(pl.multiple_of(c * ROWS, ROWS), ROWS)

    def from_x(c):
        return pltpu.make_async_copy(x.at[rows_of(c)], h.at[rows_of(c)], h_recv.at[c])

    def from_dy(c):
        return pltpu.make_async_copy(dy.at[rows_of(c)], g.at[rows_of(c)], g_recv.at[c])

    def send_h(c):
        slot = lax.rem(c, RING)
        return pltpu.make_async_remote_copy(
            src_ref=hs.at[slot],
            dst_ref=h.at[rows_of(c)],
            send_sem=h_send.at[slot],
            recv_sem=h_recv.at[c],
            device_id={"pp": lax.rem(me + 1, stages)},
            device_id_type=pl.DeviceIdType.MESH,
        )

    def send_g(c):
        slot = lax.rem(c, RING)
        return pltpu.make_async_remote_copy(
            src_ref=gs.at[slot],
            dst_ref=g.at[rows_of(c)],
            send_sem=g_send.at[slot],
            recv_sem=g_recv.at[c],
            device_id={"pp": lax.rem(me + stages - 1, stages)},
            device_id_type=pl.DeviceIdType.MESH,
        )

    @pl.when(first)
    def _():
        from_x(0).start()

    loads = (
        pltpu.make_async_copy(w_gate, wgu.at[:, pl.ds(0, ff)], w_sem.at[0]),
        pltpu.make_async_copy(w_up, wgu.at[:, pl.ds(ff, ff)], w_sem.at[1]),
        pltpu.make_async_copy(w_down, wd, w_sem.at[2]),
    )
    for load in loads:
        load.start()

    barrier = pltpu.get_barrier_semaphore()
    for other in (lax.rem(me + 1, stages), lax.rem(me + stages - 1, stages)):
        pl.semaphore_signal(barrier, inc=1, device_id={"pp": other}, device_id_type=pl.DeviceIdType.MESH)

    @pl.when(first)
    def _():
        @pl.loop(1, chunks)
        def _(c):
            from_x(c).start()

    @pl.when(last)
    def _():
        @pl.loop(0, chunks)
        def _(c):
            from_dy(c).start()

    def clear():
        acc_gu[...] = jnp.zeros_like(acc_gu)
        acc_d[...] = jnp.zeros_like(acc_d)

    for load in loads:
        load.wait()

    @pl.when(jnp.logical_not(first))
    def _():
        clear()
        transpose_gate_up(wgu, wgut)
        transpose_down(wd, wdt)

    pl.semaphore_wait(barrier, 2)

    early = tokens // 2

    def spare(i):
        return lax.rem(chunks + i, SLOTS)

    def bands_of(j):
        return pl.ds(pl.multiple_of(j * band, band), band), pl.ds(pl.multiple_of(j * tall, tall), tall)

    def terms(m, j, start, size):
        rows, tall_rows = bands_of(j)
        of_all = pl.ds(pl.multiple_of(m * tokens + start, size), size)
        part = pl.ds(start, size)
        by_gu = dot_tokens(h[of_all, rows], dgu_keep[lax.rem(m, 2), part, :])
        return by_gu, dot_tokens(act_keep[lax.rem(m, blocks), part, tall_rows], g[of_all, :])

    def out_copies(j):
        slot = (micro - 2) % 2
        rows = pl.ds(pl.multiple_of(j * band, band), band)
        return (
            pltpu.make_async_copy(dgu_keep.at[slot, rows, pl.ds(0, ff)], o_gate.at[rows], o_sem.at[0, j]),
            pltpu.make_async_copy(dgu_keep.at[slot, rows, pl.ds(ff, ff)], o_up.at[rows], o_sem.at[1, j]),
        ) + tuple(
            pltpu.make_async_copy(
                act_keep.at[(micro - 2) % blocks, rows, pl.ds(i * d, d)],
                o_down.at[pl.ds(pl.multiple_of(j * tall + i * band, band), band)],
                o_sem.at[2 + i, j],
            )
            for i in range(pieces)
        )

    @pl.loop(0, chunks + LAGS[stages - 1] + per - 1)
    def _(t):
        @pl.when(t < chunks)
        def _():
            c = t
            slot = lax.rem(c, SLOTS)
            act_out = act_keep.at[lax.rem(lax.div(c, per), blocks), rows_of(lax.rem(c, per))]

            @pl.when(first)
            def _():
                from_x(c).wait()

            @pl.when(jnp.logical_not(first))
            def _():
                send_h(c).wait_recv()

            @pl.when(jnp.logical_not(last))
            def _():
                @pl.when(c >= RING)
                def _():
                    send_h(c).wait_send()

                forward_chunk(h[rows_of(c), :], wgu, wd, keep.at[slot], act_out, hs.at[lax.rem(c, RING)])
                send_h(c).start()

        @pl.when(jnp.logical_and(first, t == 2))
        def _():
            transpose_down(wd, wdt)

        @pl.when(jnp.logical_and(first, t == 3))
        def _():
            clear()

        @pl.when(jnp.logical_and(t >= lag, t < chunks + lag))
        def _():
            c = t - lag
            slot, half = lax.rem(c, SLOTS), lax.rem(lax.div(c, per), 2)
            inside = rows_of(lax.rem(c, per))

            @pl.when(last)
            def _():
                from_dy(c).wait()

            @pl.when(jnp.logical_not(last))
            def _():
                send_g(c).wait_recv()

            def backward(out):
                rows = rows_of(c)
                backward_chunk(h[rows, :], g[rows, :], wdt, wgut, keep.at[slot], h.at[rows], dgu_keep.at[half, inside], out)

            @pl.when(first)
            def _():
                backward(None)

            @pl.when(jnp.logical_not(first))
            def _():
                @pl.when(c >= RING)
                def _():
                    send_g(c).wait_send()

                back = gs.at[lax.rem(c, RING)]

                @pl.when(last)
                def _():
                    act_out = act_keep.at[lax.rem(lax.div(c, per), blocks), inside]
                    both_ways_chunk(h[rows_of(c), :], g[rows_of(c), :], wgu, wdt, wgut, h.at[rows_of(c)], act_out, dgu_keep.at[half, inside], back)

                @pl.when(jnp.logical_not(last))
                def _():
                    backward(back)

                send_g(c).start()

        u = t - lag - (per - 1)

        @pl.when(jnp.logical_and(u >= 0, u < chunks))
        def _():
            m, j = lax.div(u, per), lax.rem(u, per)
            final = m == micro - 1

            def finish(by_gu, by_d):
                rows, tall_rows = bands_of(j)
                dgu_keep[(micro - 2) % 2, rows, :] = (acc_gu[rows, :] + by_gu.astype(BF16).astype(F32)).astype(BF16)
                total = (acc_d[tall_rows, :] + by_d.astype(BF16).astype(F32)).astype(BF16)
                for i in range(pieces):
                    act_keep[(micro - 2) % blocks, rows, i * d : (i + 1) * d] = total[i * band : (i + 1) * band, :]
                for copy in out_copies(j):
                    copy.start()

            @pl.when(jnp.logical_not(final))
            def _():
                rows, tall_rows = bands_of(j)
                by_gu, by_d = terms(m, j, 0, tokens)
                acc_gu[rows, :] += by_gu.astype(BF16).astype(F32)
                acc_d[tall_rows, :] += by_d.astype(BF16).astype(F32)

            @pl.when(jnp.logical_and(final, jnp.logical_not(first)))
            def _():
                finish(*terms(m, j, 0, tokens))

            @pl.when(jnp.logical_and(final, first))
            def _():
                by_gu, by_d = terms(m, j, early, tokens - early)
                held = keep[spare(2 * j + 1)]
                part = jnp.concatenate([held[:, i * d : (i + 1) * d] for i in range(pieces)], axis=0)
                finish(keep[spare(2 * j)] + by_gu, part + by_d)

        e = u - (chunks - per) + per // 2

        @pl.when(jnp.logical_and(first, jnp.logical_and(e >= 0, e < per // 2)))
        def _():
            for j in (2 * e, 2 * e + 1):
                by_gu, by_d = terms(micro - 1, j, 0, early)
                keep[spare(2 * j)] = by_gu
                for i in range(pieces):
                    keep[spare(2 * j + 1), :, i * d : (i + 1) * d] = by_d[i * band : (i + 1) * band, :]

    @pl.loop(0, min(RING, chunks))
    def _(c):
        @pl.when(jnp.logical_not(last))
        def _():
            send_h(c).wait_send()

        @pl.when(jnp.logical_not(first))
        def _():
            send_g(c).wait_send()

    @pl.loop(0, per)
    def _(j):
        for copy in out_copies(j):
            copy.wait()


def hand_over(per, *refs):
    ins, outs, held, sem = refs[:3], refs[3:6], refs[6:9], refs[9]
    moves = []
    for j in range(per):
        for i in range(3):
            size = ins[i].shape[0] // per
            rows = pl.ds(j * size, size)
            moves.append(
                (
                    pltpu.make_async_copy(ins[i].at[rows], held[i].at[0, rows], sem.at[0, i, j]),
                    pltpu.make_async_copy(held[i].at[0, rows], outs[i].at[0, rows], sem.at[1, i, j]),
                )
            )
    for take, _ in moves:
        take.start()
    for take, put in moves:
        take.wait()
        put.start()
    for _, put in moves:
        put.wait()


def solution(mesh):
    stages = mesh.shape["pp"]

    def step(x, dy, w_gate, w_up, w_down):
        micro, tokens, d = x.shape
        ff = w_gate.shape[-1]
        assert w_gate.shape[0] == 1
        per = tokens // ROWS
        chunks = micro * per
        blocks = (LAGS[stages - 1] + 2 * per - 2) // per + 1
        anywhere = pl.BlockSpec(memory_space=pl.ANY)
        tall = jax.ShapeDtypeStruct((d, ff), BF16)
        by_gate, by_up, by_down = pl.pallas_call(
            functools.partial(kernel, stages, micro, tokens),
            out_shape=(tall, tall, jax.ShapeDtypeStruct((ff, d), BF16)),
            in_specs=[anywhere] * 5,
            out_specs=(anywhere,) * 3,
            scratch_shapes=[
                pltpu.VMEM((d, 2 * ff), BF16),
                pltpu.VMEM((ff, d), BF16),
                pltpu.VMEM((2 * ff, d), BF16),
                pltpu.VMEM((d, ff), BF16),
                pltpu.VMEM((micro * tokens, d), BF16),
                pltpu.VMEM((micro * tokens, d), BF16),
                pltpu.VMEM((RING, ROWS, d), BF16),
                pltpu.VMEM((RING, ROWS, d), BF16),
                pltpu.VMEM((SLOTS, ROWS, 2 * ff), F32),
                pltpu.VMEM((blocks, tokens, ff), BF16),
                pltpu.VMEM((2, tokens, 2 * ff), BF16),
                pltpu.VMEM((d, 2 * ff), F32),
                pltpu.VMEM((ff, d), F32),
                pltpu.SemaphoreType.DMA((3,)),
                pltpu.SemaphoreType.DMA((2 + ff // d, per)),
                pltpu.SemaphoreType.DMA((chunks,)),
                pltpu.SemaphoreType.DMA((chunks,)),
                pltpu.SemaphoreType.DMA((RING,)),
                pltpu.SemaphoreType.DMA((RING,)),
            ],
            compiler_params=pltpu.CompilerParams(collective_id=0, has_side_effects=True, vmem_limit_bytes=67043328),
        )(x.reshape(micro * tokens, d), dy.reshape(micro * tokens, d), w_gate[0], w_up[0], w_down[0])
        shapes = ((1, d, ff), (1, d, ff), (1, ff, d))
        return pl.pallas_call(
            functools.partial(hand_over, per),
            out_shape=tuple(jax.ShapeDtypeStruct(shape, BF16) for shape in shapes),
            in_specs=[anywhere] * 3,
            out_specs=(anywhere,) * 3,
            scratch_shapes=[pltpu.VMEM(shape, BF16) for shape in shapes] + [pltpu.SemaphoreType.DMA((2, 3, per))],
        )(by_gate, by_up, by_down)

    return jax.shard_map(
        step,
        mesh=mesh,
        in_specs=(P("rep", None, None),) * 2 + (P("pp", None, None),) * 3,
        out_specs=(P(("rep", "pp"), None, None),) * 3,
        check_vma=False,
    )
```

```python
import functools

import jax
import jax.numpy as jnp
from jax import lax
from jax.experimental import pallas as pl
from jax.experimental.pallas import tpu as pltpu
from jax.sharding import PartitionSpec as P

F32, BF16 = jnp.float32, jnp.bfloat16
ROWS = 128
LAGS = (0, 4, 8, 13)
SLOTS = max(LAGS) + 1
RING = 3
LANES = 128


def dot(a, b):
    return jnp.dot(a, b, preferred_element_type=F32)


def dot_tokens(a, b):
    return lax.dot_general(a, b, (((0,), (0,)), ((), ())), preferred_element_type=F32)


def scale_of(wide):
    return lax.rsqrt(jnp.mean(wide * wide, -1, keepdims=True) + 1e-6)


def sigmoid(v):
    return 0.5 * jnp.tanh(0.5 * v) + 0.5


def transpose_down(wd, wdt):
    @pl.loop(0, wd.shape[0] // LANES)
    def _(i):
        part = pl.ds(pl.multiple_of(i * LANES, LANES), LANES)
        wdt[:, part] = wd[part, :].T


def transpose_gate_up(wgu, wgut):
    @pl.loop(0, wgu.shape[1] // LANES)
    def _(i):
        part = pl.ds(pl.multiple_of(i * LANES, LANES), LANES)
        wgut[part, :] = wgu[:, part].T


def forward_chunk(hc, wgu, wd, keep, act_out, out):
    ff = wd.shape[0]
    wide = hc.astype(F32)
    a = (wide * scale_of(wide)).astype(BF16)
    acts = []
    width = ff // 6
    for i in range(6):
        lo, hi = i * width, (i + 1) * width
        gate = dot(a, wgu[:, lo:hi])
        up = dot(a, wgu[:, ff + lo : ff + hi])
        sig = sigmoid(gate)
        silu = gate * sig
        act = (silu * up).astype(BF16)
        act_out[:, lo:hi] = act
        keep[:, lo:hi] = up * (sig + silu * (1.0 - sig))
        keep[:, ff + lo : ff + hi] = silu
        acts.append(act)
    if out is not None:
        out[...] = hc + dot(jnp.concatenate(acts, axis=1), wd[...]).astype(BF16)


def backward_chunk(hc, gc, wdt, wgut, keep, a_out, dgu_out, out):
    ff = wdt.shape[1]
    wide = hc.astype(F32)
    scale = scale_of(wide)
    gates, ups = [], []
    width = ff // 3
    for i in range(3):
        lo, hi = i * width, (i + 1) * width
        d = dot(gc, wdt[:, lo:hi]).astype(BF16).astype(F32)
        by_gate = (d * keep[:, lo:hi]).astype(BF16)
        by_up = (d * keep[:, ff + lo : ff + hi]).astype(BF16)
        dgu_out[:, lo:hi] = by_gate
        dgu_out[:, ff + lo : ff + hi] = by_up
        gates.append(by_gate)
        ups.append(by_up)
    a_out[...] = (wide * scale).astype(BF16)
    if out is not None:
        send_back(gc, wide, scale, gates, ups, wgut, out)


def both_ways_chunk(hc, gc, wgu, wdt, wgut, a_out, act_out, dgu_out, out):
    ff = wdt.shape[1]
    wide = hc.astype(F32)
    scale = scale_of(wide)
    a = (wide * scale).astype(BF16)
    gates, ups = [], []
    width = ff // 6
    for i in range(6):
        lo, hi = i * width, (i + 1) * width
        gate = dot(a, wgu[:, lo:hi])
        up = dot(a, wgu[:, ff + lo : ff + hi])
        d = dot(gc, wdt[:, lo:hi]).astype(BF16).astype(F32)
        sig = sigmoid(gate)
        silu = gate * sig
        act_out[:, lo:hi] = (silu * up).astype(BF16)
        by_gate = (d * (up * (sig + silu * (1.0 - sig)))).astype(BF16)
        by_up = (d * silu).astype(BF16)
        dgu_out[:, lo:hi] = by_gate
        dgu_out[:, ff + lo : ff + hi] = by_up
        gates.append(by_gate)
        ups.append(by_up)
    a_out[...] = a
    send_back(gc, wide, scale, gates, ups, wgut, out)


def send_back(gc, wide, scale, gates, ups, wgut, out):
    half = wgut.shape[0] // 2
    by_a = dot(jnp.concatenate(gates, axis=1), wgut[:half, :]).astype(BF16) + dot(jnp.concatenate(ups, axis=1), wgut[half:, :]).astype(BF16)
    by_a = by_a.astype(F32)
    inner = jnp.sum(by_a * wide, -1, keepdims=True) * (scale * scale * scale * (1.0 / wide.shape[-1]))
    out[...] = gc + (by_a * scale - wide * inner).astype(BF16)


def kernel(
    stages,
    micro,
    tokens,
    x,
    dy,
    w_gate,
    w_up,
    w_down,
    o_gate,
    o_up,
    o_down,
    wgu,
    wd,
    wgut,
    wdt,
    h,
    g,
    hs,
    gs,
    keep,
    act_keep,
    dgu_keep,
    acc_gu,
    acc_d,
    w_sem,
    o_sem,
    h_recv,
    g_recv,
    h_send,
    g_send,
):
    me = lax.axis_index("pp")
    first, last = me == 0, me == stages - 1
    ff = wd.shape[0]
    per = tokens // ROWS
    chunks = micro * per
    d = wgu.shape[0]
    band, tall = d // per, ff // per
    pieces = ff // d
    behind = stages - 1 - me
    lag = sum(jnp.where(behind == i, LAGS[i], 0) for i in range(stages))
    blocks = act_keep.shape[0]

    def rows_of(c):
        return pl.ds(pl.multiple_of(c * ROWS, ROWS), ROWS)

    def from_x(c):
        return pltpu.make_async_copy(x.at[rows_of(c)], h.at[rows_of(c)], h_recv.at[c])

    def from_dy(c):
        return pltpu.make_async_copy(dy.at[rows_of(c)], g.at[rows_of(c)], g_recv.at[c])

    def send_h(c):
        slot = lax.rem(c, RING)
        return pltpu.make_async_remote_copy(
            src_ref=hs.at[slot],
            dst_ref=h.at[rows_of(c)],
            send_sem=h_send.at[slot],
            recv_sem=h_recv.at[c],
            device_id={"pp": lax.rem(me + 1, stages)},
            device_id_type=pl.DeviceIdType.MESH,
        )

    def send_g(c):
        slot = lax.rem(c, RING)
        return pltpu.make_async_remote_copy(
            src_ref=gs.at[slot],
            dst_ref=g.at[rows_of(c)],
            send_sem=g_send.at[slot],
            recv_sem=g_recv.at[c],
            device_id={"pp": lax.rem(me + stages - 1, stages)},
            device_id_type=pl.DeviceIdType.MESH,
        )

    ahead = 2

    @pl.when(first)
    def _():
        for c in range(ahead):
            from_x(c).start()

    loads = (
        pltpu.make_async_copy(w_gate, wgu.at[:, pl.ds(0, ff)], w_sem.at[0]),
        pltpu.make_async_copy(w_up, wgu.at[:, pl.ds(ff, ff)], w_sem.at[1]),
        pltpu.make_async_copy(w_down, wd, w_sem.at[2]),
    )
    for load in loads:
        load.start()

    barrier = pltpu.get_barrier_semaphore()
    for other in (lax.rem(me + 1, stages), lax.rem(me + stages - 1, stages)):
        pl.semaphore_signal(barrier, inc=1, device_id={"pp": other}, device_id_type=pl.DeviceIdType.MESH)

    def clear():
        acc_gu[...] = jnp.zeros_like(acc_gu)
        acc_d[...] = jnp.zeros_like(acc_d)

    for load in loads:
        load.wait()

    @pl.when(first)
    def _():
        @pl.loop(ahead, chunks)
        def _(c):
            from_x(c).start()

    @pl.when(last)
    def _():
        @pl.loop(0, chunks)
        def _(c):
            from_dy(c).start()

    @pl.when(jnp.logical_not(first))
    def _():
        clear()
        transpose_gate_up(wgu, wgut)
        transpose_down(wd, wdt)

    pl.semaphore_wait(barrier, 2)

    early = tokens // 2

    def spare(i):
        return lax.rem(chunks + i, SLOTS)

    def bands_of(j):
        return pl.ds(pl.multiple_of(j * band, band), band), pl.ds(pl.multiple_of(j * tall, tall), tall)

    def terms(m, j, start, size):
        rows, tall_rows = bands_of(j)
        of_all = pl.ds(pl.multiple_of(m * tokens + start, size), size)
        part = pl.ds(start, size)
        by_gu = dot_tokens(h[of_all, rows], dgu_keep[lax.rem(m, 2), part, :])
        return by_gu, dot_tokens(act_keep[lax.rem(m, blocks), part, tall_rows], g[of_all, :])

    def out_copies(j):
        slot = (micro - 2) % 2
        rows = pl.ds(pl.multiple_of(j * band, band), band)
        return (
            pltpu.make_async_copy(dgu_keep.at[slot, rows, pl.ds(0, ff)], o_gate.at[rows], o_sem.at[0, j]),
            pltpu.make_async_copy(dgu_keep.at[slot, rows, pl.ds(ff, ff)], o_up.at[rows], o_sem.at[1, j]),
        ) + tuple(
            pltpu.make_async_copy(
                act_keep.at[(micro - 2) % blocks, rows, pl.ds(i * d, d)],
                o_down.at[pl.ds(pl.multiple_of(j * tall + i * band, band), band)],
                o_sem.at[2 + i, j],
            )
            for i in range(pieces)
        )

    @pl.loop(0, chunks + LAGS[stages - 1] + per - 1)
    def _(t):
        @pl.when(t < chunks)
        def _():
            c = t
            slot = lax.rem(c, SLOTS)
            act_out = act_keep.at[lax.rem(lax.div(c, per), blocks), rows_of(lax.rem(c, per))]

            @pl.when(first)
            def _():
                from_x(c).wait()

            @pl.when(jnp.logical_not(first))
            def _():
                send_h(c).wait_recv()

            @pl.when(jnp.logical_not(last))
            def _():
                @pl.when(c >= RING)
                def _():
                    send_h(c).wait_send()

                forward_chunk(h[rows_of(c), :], wgu, wd, keep.at[slot], act_out, hs.at[lax.rem(c, RING)])
                send_h(c).start()

        @pl.when(jnp.logical_and(first, t == 2))
        def _():
            transpose_down(wd, wdt)

        @pl.when(jnp.logical_and(first, t == 3))
        def _():
            clear()

        @pl.when(jnp.logical_and(t >= lag, t < chunks + lag))
        def _():
            c = t - lag
            slot, half = lax.rem(c, SLOTS), lax.rem(lax.div(c, per), 2)
            inside = rows_of(lax.rem(c, per))

            @pl.when(last)
            def _():
                from_dy(c).wait()

            @pl.when(jnp.logical_not(last))
            def _():
                send_g(c).wait_recv()

            def backward(out):
                rows = rows_of(c)
                backward_chunk(h[rows, :], g[rows, :], wdt, wgut, keep.at[slot], h.at[rows], dgu_keep.at[half, inside], out)

            @pl.when(first)
            def _():
                backward(None)

            @pl.when(jnp.logical_not(first))
            def _():
                @pl.when(c >= RING)
                def _():
                    send_g(c).wait_send()

                back = gs.at[lax.rem(c, RING)]

                @pl.when(last)
                def _():
                    act_out = act_keep.at[lax.rem(lax.div(c, per), blocks), inside]
                    both_ways_chunk(h[rows_of(c), :], g[rows_of(c), :], wgu, wdt, wgut, h.at[rows_of(c)], act_out, dgu_keep.at[half, inside], back)

                @pl.when(jnp.logical_not(last))
                def _():
                    backward(back)

                send_g(c).start()

        u = t - lag - (per - 1)

        @pl.when(jnp.logical_and(u >= 0, u < chunks))
        def _():
            m, j = lax.div(u, per), lax.rem(u, per)
            final = m == micro - 1

            def finish(j, by_gu, by_d):
                rows, tall_rows = bands_of(j)
                dgu_keep[(micro - 2) % 2, rows, :] = (acc_gu[rows, :] + by_gu.astype(BF16).astype(F32)).astype(BF16)
                total = (acc_d[tall_rows, :] + by_d.astype(BF16).astype(F32)).astype(BF16)
                for i in range(pieces):
                    act_keep[(micro - 2) % blocks, rows, i * d : (i + 1) * d] = total[i * band : (i + 1) * band, :]
                for copy in out_copies(j):
                    copy.start()

            @pl.when(jnp.logical_not(final))
            def _():
                rows, tall_rows = bands_of(j)
                by_gu, by_d = terms(m, j, 0, tokens)
                acc_gu[rows, :] += by_gu.astype(BF16).astype(F32)
                acc_d[tall_rows, :] += by_d.astype(BF16).astype(F32)

            @pl.when(jnp.logical_and(final, jnp.logical_not(first)))
            def _():
                finish(j, *terms(m, j, 0, tokens))

            @pl.when(jnp.logical_and(jnp.logical_and(final, first), j < per // 2))
            def _():
                for b in (2 * j, 2 * j + 1):
                    by_gu, by_d = terms(m, b, early, tokens - early)
                    held = keep[spare(2 * b + 1)]
                    part = jnp.concatenate([held[:, i * d : (i + 1) * d] for i in range(pieces)], axis=0)
                    finish(b, keep[spare(2 * b)] + by_gu, part + by_d)

        e = u - (chunks - per) + per // 2

        @pl.when(jnp.logical_and(first, jnp.logical_and(e >= 0, e < per // 2)))
        def _():
            for j in (2 * e, 2 * e + 1):
                by_gu, by_d = terms(micro - 1, j, 0, early)
                keep[spare(2 * j)] = by_gu
                for i in range(pieces):
                    keep[spare(2 * j + 1), :, i * d : (i + 1) * d] = by_d[i * band : (i + 1) * band, :]

    @pl.loop(0, min(RING, chunks))
    def _(c):
        @pl.when(jnp.logical_not(last))
        def _():
            send_h(c).wait_send()

        @pl.when(jnp.logical_not(first))
        def _():
            send_g(c).wait_send()

    @pl.loop(0, per)
    def _(j):
        for copy in out_copies(j):
            copy.wait()


def hand_over(per, *refs):
    ins, outs, held, sem = refs[:3], refs[3:6], refs[6:9], refs[9]
    moves = []
    for j in range(per):
        for i in range(3):
            size = ins[i].shape[0] // per
            rows = pl.ds(j * size, size)
            moves.append(
                (
                    pltpu.make_async_copy(ins[i].at[rows], held[i].at[0, rows], sem.at[0, i, j]),
                    pltpu.make_async_copy(held[i].at[0, rows], outs[i].at[0, rows], sem.at[1, i, j]),
                )
            )
    for take, _ in moves:
        take.start()
    for take, put in moves:
        take.wait()
        put.start()
    for _, put in moves:
        put.wait()


def solution(mesh):
    stages = mesh.shape["pp"]

    def step(x, dy, w_gate, w_up, w_down):
        micro, tokens, d = x.shape
        ff = w_gate.shape[-1]
        assert w_gate.shape[0] == 1
        per = tokens // ROWS
        chunks = micro * per
        blocks = (LAGS[stages - 1] + 2 * per - 2) // per + 1
        anywhere = pl.BlockSpec(memory_space=pl.ANY)
        tall = jax.ShapeDtypeStruct((d, ff), BF16)
        by_gate, by_up, by_down = pl.pallas_call(
            functools.partial(kernel, stages, micro, tokens),
            out_shape=(tall, tall, jax.ShapeDtypeStruct((ff, d), BF16)),
            in_specs=[anywhere] * 5,
            out_specs=(anywhere,) * 3,
            scratch_shapes=[
                pltpu.VMEM((d, 2 * ff), BF16),
                pltpu.VMEM((ff, d), BF16),
                pltpu.VMEM((2 * ff, d), BF16),
                pltpu.VMEM((d, ff), BF16),
                pltpu.VMEM((micro * tokens, d), BF16),
                pltpu.VMEM((micro * tokens, d), BF16),
                pltpu.VMEM((RING, ROWS, d), BF16),
                pltpu.VMEM((RING, ROWS, d), BF16),
                pltpu.VMEM((SLOTS, ROWS, 2 * ff), F32),
                pltpu.VMEM((blocks, tokens, ff), BF16),
                pltpu.VMEM((2, tokens, 2 * ff), BF16),
                pltpu.VMEM((d, 2 * ff), F32),
                pltpu.VMEM((ff, d), F32),
                pltpu.SemaphoreType.DMA((3,)),
                pltpu.SemaphoreType.DMA((2 + ff // d, per)),
                pltpu.SemaphoreType.DMA((chunks,)),
                pltpu.SemaphoreType.DMA((chunks,)),
                pltpu.SemaphoreType.DMA((RING,)),
                pltpu.SemaphoreType.DMA((RING,)),
            ],
            compiler_params=pltpu.CompilerParams(collective_id=0, has_side_effects=True, vmem_limit_bytes=67043328),
        )(x.reshape(micro * tokens, d), dy.reshape(micro * tokens, d), w_gate[0], w_up[0], w_down[0])
        shapes = ((1, d, ff), (1, d, ff), (1, ff, d))
        return pl.pallas_call(
            functools.partial(hand_over, per),
            out_shape=tuple(jax.ShapeDtypeStruct(shape, BF16) for shape in shapes),
            in_specs=[anywhere] * 3,
            out_specs=(anywhere,) * 3,
            scratch_shapes=[pltpu.VMEM(shape, BF16) for shape in shapes] + [pltpu.SemaphoreType.DMA((2, 3, per))],
        )(by_gate, by_up, by_down)

    return jax.shard_map(
        step,
        mesh=mesh,
        in_specs=(P("rep", None, None),) * 2 + (P("pp", None, None),) * 3,
        out_specs=(P(("rep", "pp"), None, None),) * 3,
        check_vma=False,
    )
```
